32 devices in a mesh: band: 8 (over z, y), grid: 4 (over x, core).
Axes of the slice: x: 2, y: 2, z: 4, core: 2. Of those that a mesh axis runs over, the one named last changes fastest.
Arguments:
- own_bands: float32 [32, 128, 128, 128], P('band', 'grid'), may hold values from -1.5 to 1.5
- travel_bands: float32 [32, 128, 128, 128], P('band', 'grid'), may hold values from -1.5 to 1.5
Outputs:
- own_terms: float32 [32, 128, 128, 128], P('band', 'grid')
- partner_terms: float32 [32, 128, 128, 128], P('band', 'grid')
The draws below stay inside these ranges and needn't reach their ends.
All inputs are finite; a program needn't handle non-finite values.
Results may differ from the reference program's by a relative error of at most 0.00011.
Values sent between devices are 32-bit elements; how exact they have to be, the bound alone decides.
A program may use at most 192 MiB of HBM per device.

```python
import math
import jax
import jax.numpy as jnp
from jax import lax

NX = 128
NY = 128
NZ = 128
OWN = 4
VIS = 4
BANDS = 32
TRAVEL = 32
N_BAND = 8


def band_field(base_key, band_count):
    return 0.5 * jax.random.truncated_normal(jax.random.fold_in(base_key, 4), -3.0, 3.0, (band_count, NZ, NY, NX), jnp.float32)


def draw_own_bands(key, part):
    return band_field(jax.random.fold_in(key, 11), BANDS)


def draw_travel_bands(key, part):
    return band_field(jax.random.fold_in(key, 23), TRAVEL)


def setup_inputs(seed: int = 0) -> dict:
    streams_of = jax.random.split(jax.random.key(seed), 3)
    return {
        "own_bands": draw_own_bands(jax.random.fold_in(streams_of[2], 71), 0),
        "travel_bands": draw_travel_bands(jax.random.fold_in(streams_of[2], 71), 0),
    }


FRACTION = 0.25


def wave_square(points, first_row, length):
    position = first_row + jnp.arange(points, dtype=jnp.int32)
    position = (position + length // 2) % length - length // 2
    wavenumber = (2.0 * math.pi / length) * position.astype(jnp.float32)
    return wavenumber * wavenumber


def coulomb(first_row, row_count):
    squared = wave_square(NZ, 0, NZ)[:, None, None] + wave_square(row_count, first_row, NY)[None, :, None] + wave_square(NX, 0, NX)[None, None, :]
    safe_square = jnp.where(squared > 0.0, squared, 1.0)
    return jnp.where(squared > 0.0, 4.0 * math.pi / safe_square, 0.0)


def reference(own_bands, travel_bands):
    kernel = coulomb(0, NY)[:, :, : NX // 2 + 1]
    owned_groups = own_bands.reshape(N_BAND, OWN, NZ, NY, NX)
    arrived = jnp.roll(travel_bands.reshape(N_BAND, VIS, NZ, NY, NX), 1, axis=0)

    def group_terms(blocks):
        owned, visitors = blocks

        def visit_band(accumulated, visitor):
            density = owned * visitor
            potential = jnp.fft.irfftn(kernel * jnp.fft.rfftn(density, axes=(1, 2, 3)), s=(NZ, NY, NX), axes=(1, 2, 3))
            return accumulated + potential * visitor, jnp.sum(potential * owned, axis=0)

        accumulated, partner = lax.scan(visit_band, jnp.zeros_like(owned), visitors)
        return -FRACTION * accumulated, -FRACTION * partner

    own_terms, held = lax.map(group_terms, (owned_groups, arrived))
    held = jnp.roll(held, -1, axis=0)
    return own_terms.reshape(BANDS, NZ, NY, NX), held.reshape(TRAVEL, NZ, NY, NX)
```

```python
import math

import jax
import jax.numpy as jnp
from jax import lax
from jax.sharding import PartitionSpec as P

NX = 128
NY = 128
NZ = 128


FRACTION = 0.25
HIGHEST_PRECISION = lax.Precision.HIGHEST


def passed_along(block, axis, distance):
    devices = range(lax.axis_size(axis))
    route = [((i - distance) % len(devices), i) for i in devices]
    return lax.ppermute(block, axis, route)


def wave_square(points, first_row, length):
    position = first_row + jnp.arange(points, dtype=jnp.int32)
    position = (position + length // 2) % length - length // 2
    wavenumber = 2.0 * math.pi / length * position.astype(jnp.float32)
    return wavenumber * wavenumber


def coulomb(first_row, row_count):
    squared = (
        wave_square(NZ, 0, NZ)[:, None, None]
        + wave_square(row_count, first_row, NY)[None, :, None]
        + wave_square(NX, 0, NX)[None, None, :]
    )
    safe_square = jnp.where(squared > 0.0, squared, 1.0)
    return jnp.where(squared > 0.0, 4.0 * math.pi / safe_square, 0.0)


def fourier_table(length, inverse):
    position = jnp.arange(length, dtype=jnp.int32)
    phase_turns = position[:, None] * position[None, :] % length
    phase_angle = 2.0 * math.pi / length * phase_turns.astype(jnp.float32)
    cosine = jnp.cos(phase_angle)
    sine_part = jnp.sin(phase_angle)
    norm_factor = 1.0
    if inverse:
        sine_part = -sine_part
        norm_factor = 1.0 / length
    return norm_factor * jnp.stack(
        [jnp.stack([cosine, -sine_part]), jnp.stack([sine_part, cosine])]
    )


def solve_pairs(packed, kernel_slab):
    spectrum = jnp.einsum(
        "pczyx,cdxk->dpzyk", packed, fourier_table(NX, False), precision=HIGHEST_PRECISION
    )
    spectrum = jnp.einsum(
        "cpzyx,cdyk->dpzkx", spectrum, fourier_table(NY, False), precision=HIGHEST_PRECISION
    )
    forward_z = fourier_table(NZ, False)
    inverse_z = fourier_table(NZ, True)
    screened = (
        jnp.einsum(
            "cpzyx,cdzk->dpkyx",
            lax.all_to_all(spectrum, "grid", split_axis=3, concat_axis=2, tiled=True),
            forward_z,
            precision=HIGHEST_PRECISION,
        )
        * kernel_slab
    )
    screened = jnp.einsum("cpzyx,cdzk->dpkyx", screened, inverse_z, precision=HIGHEST_PRECISION)
    planes = lax.all_to_all(screened, "grid", split_axis=2, concat_axis=3, tiled=True)
    planes = jnp.einsum(
        "cpzyx,cdyk->dpzkx", planes, fourier_table(NY, True), precision=HIGHEST_PRECISION
    )
    return jnp.einsum(
        "cpzyx,cdxk->pdzyk", planes, fourier_table(NX, True), precision=HIGHEST_PRECISION
    )


def pair_terms(owned, visitors, kernel_slab):
    count_vis = visitors.shape[0]
    count_own = owned.shape[0]
    density = owned[None] * visitors[:, None]
    packed = density.reshape((count_vis * count_own // 2, 2) + owned.shape[1:])
    potential = solve_pairs(packed, kernel_slab).reshape(density.shape)
    own_part = jnp.sum(potential * visitors[:, None], axis=0)
    partner = jnp.sum(potential * owned[None], axis=1)
    return (own_part, partner)


def body(own_bands, travel_bands):
    rows_local = NY // lax.axis_size("grid")
    kernel_slab = coulomb(lax.axis_index("grid") * rows_local, rows_local)
    count_vis = travel_bands.shape[0]
    own_total = jnp.zeros_like(own_bands)
    returned = []
    for visit_index in range(count_vis):
        visitor = passed_along(travel_bands[visit_index : visit_index + 1], "band", 1)
        own_part, partner = pair_terms(own_bands, visitor, kernel_slab)
        own_total = own_total + own_part
        returned.append(passed_along(partner, "band", -1))
    partner_total = jnp.concatenate(returned, axis=0)
    return (-FRACTION * own_total, -FRACTION * partner_total)


def exchanged(block, bit):
    devices = range(lax.axis_size("grid"))
    return lax.ppermute(block, "grid", [(i, i ^ bit) for i in devices])


def line_table(from_position, to_position, length, inverse):
    phase_turns = from_position[:, None] * to_position[None, :] % length
    phase_angle = 2.0 * math.pi / length * phase_turns.astype(jnp.float32)
    cosine = jnp.cos(phase_angle)
    sine_part = jnp.sin(phase_angle)
    norm_factor = 1.0
    if inverse:
        sine_part = -sine_part
        norm_factor = 1.0 / length
    return norm_factor * jnp.stack(
        [jnp.stack([cosine, -sine_part]), jnp.stack([sine_part, cosine])]
    )


def transform(equation, values, table):
    return jnp.einsum(equation, values, table, precision=lax.Precision.HIGH)


def square_body(own_bands, travel_bands):
    rank = lax.axis_index("grid")
    chip, core = rank // 2, rank % 2
    half_own = own_bands.shape[0] // 2
    half_vis = travel_bands.shape[0] // 2
    depth, ny, nx = own_bands.shape[1:]
    nz = depth * lax.axis_size("grid")

    def planes(first, second):
        steps = jnp.arange(depth, dtype=jnp.int32)
        return jnp.concatenate([first * depth + steps, second * depth + steps])

    every_z = jnp.arange(nz, dtype=jnp.int32)
    every_y = jnp.arange(ny, dtype=jnp.int32)
    every_x = jnp.arange(nx, dtype=jnp.int32)
    piece_z = (planes(rank, rank ^ 1), planes(rank ^ 2, rank ^ 3))
    forward_x = line_table(every_x, every_x, nx, False)
    forward_y = line_table(every_y, every_y, ny, False)
    inverse_x = line_table(every_x, every_x, nx, True)
    inverse_y = line_table(every_y, every_y, ny, True)
    forward_z = [line_table(z, every_z, nz, False) for z in piece_z]
    inverse_z = [line_table(every_z, z, nz, True) for z in piece_z]
    kernel_cube = coulomb(0, ny)

    own_mine = lax.dynamic_slice_in_dim(own_bands, chip * half_own, half_own, 0)
    own_away = lax.dynamic_slice_in_dim(own_bands, (1 - chip) * half_own, half_own, 0)
    own_far = exchanged(own_away, 2)
    owned = [
        jnp.concatenate([block, exchanged(block, 1)], axis=1) for block in (own_mine, own_far)
    ]

    visitors = []
    for k in range(half_vis):
        mine = lax.dynamic_index_in_dim(travel_bands, core * half_vis + k, 0, keepdims=False)
        away = lax.dynamic_index_in_dim(travel_bands, (1 - core) * half_vis + k, 0, keepdims=False)
        away = passed_along(away, "band", 1)
        mine = passed_along(mine, "band", 1)
        away = exchanged(away, 1)
        visitors.append(
            [
                jnp.concatenate([mine, away], axis=0),
                jnp.concatenate([exchanged(mine, 2), exchanged(away, 2)], axis=0),
            ]
        )

    own_sum = [0.0, 0.0]
    held_mine, held_away = [], []
    for k in range(half_vis):
        spectrum = 0.0
        for p in (0, 1):
            part = owned[p] * visitors[k][p][None]
            part = transform("czyx,cdxk->dzyk", part, forward_x)
            part = transform("czyx,cdyk->dzkx", part, forward_y)
            spectrum = spectrum + transform("czyx,cdzk->dkyx", part, forward_z[p])
        spectrum = spectrum * kernel_cube
        held = [None, None]
        for p in (1, 0):
            part = transform("czyx,cdzk->dkyx", spectrum, inverse_z[p])
            part = transform("czyx,cdyk->dzkx", part, inverse_y)
            part = transform("czyx,cdxk->dzyk", part, inverse_x)
            held[p] = jnp.sum(part * owned[p], axis=0)
            own_sum[p] = own_sum[p] + part * visitors[k][p][None]
        held_near = -FRACTION * (held[0] + exchanged(held[1], 2))
        held_mine.append(passed_along(held_near[:depth], "band", -1))
        held_away.append(passed_along(exchanged(held_near[depth:], 1), "band", -1))

    own_near, own_back = [
        -FRACTION * (total[:, :depth] + exchanged(total[:, depth:], 1)) for total in own_sum
    ]
    own_back = exchanged(own_back, 2)
    own_rows = jnp.where(
        chip == 0,
        jnp.concatenate([own_near, own_back], axis=0),
        jnp.concatenate([own_back, own_near], axis=0),
    )
    held_rows = jnp.where(
        core == 0, jnp.stack(held_mine + held_away), jnp.stack(held_away + held_mine)
    )
    return own_rows, held_rows


def solution(mesh):
    in_specs = (P("band", "grid", None, None), P("band", "grid", None, None))
    out_specs = (P("band", "grid", None, None), P("band", "grid", None, None))

    def placed(own_bands, travel_bands):
        group_own = own_bands.shape[0] // mesh.shape["band"]
        group_vis = travel_bands.shape[0] // mesh.shape["band"]
        square = mesh.shape["grid"] == 4 and group_own == 4 and group_vis % 2 == 0
        return jax.shard_map(
            square_body if square else body,
            mesh=mesh,
            in_specs=in_specs,
            out_specs=out_specs,
            check_vma=False,
        )(own_bands, travel_bands)

    return placed
```
